32 devices in a mesh: study: 2 (over x), ky: 16 (over z, y, core).
Axes of the slice: x: 2, y: 2, z: 4, core: 2. Of those that a mesh axis runs over, the one named last changes fastest.
Arguments:
- kspace: bfloat16 [32, 2, 32, 256, 256], P('study', None, None, 'ky'), parts along dimension 0, may hold values from -6 to 6
- kernel: bfloat16 [2, 768, 64], replicated, may hold values from -0.21875 to 0.21875
- pattern: int32 [32], P('study'), parts along dimension 0, may hold values from 0 to 2
- offsets: int32 [4], replicated, may hold values from -2 to 2
- segment: int32 [256], replicated, may hold values from 0 to 2
- temporal_basis: float32 [5, 16], replicated, may hold values from -1.5 to 1.5
Outputs:
- basis_images: float32 [10, 2, 32, 256, 256], P('study', None, None, 'ky'), parts along dimension 0
The draws below stay inside these ranges and needn't reach their ends.
There are 2 independent parts, one for each index of `study`. The reference program is written for one: setup_inputs(seed, part) draws one part's arguments, and reference() takes and returns one part's arrays. A program takes and returns all parts, laid end to end along the dimension named above; an argument that names none is the same for every part. Nothing has to cross between parts.
All inputs are finite; a program needn't handle non-finite values.
Results may differ from the reference program's by a relative error of at most 0.0003.
Values may be sent and summed in bfloat16 or wider, within the bound.
No kernel may reach another device: no remote copies, remote signals or barrier semaphores. Data moves between devices by JAX's collectives and lax.ppermute only.
A program may use at most 192 MiB of HBM per device.

```python
import jax
import jax.numpy as jnp
from jax import lax

COILS = 32
KY = 256
KX = 256
BASIS = 5
TAPS_KY = 3
TAPS_KX = 4
GROUPS = 2
ALTERNATES = 3
FRAMES = 16
KIN = 768


def plant(drawn, rng, least, top_value):
    extent = drawn.shape
    spot = [jax.random.randint(jax.random.fold_in(rng, axis), (), 0, extent[axis]) for axis in range(len(extent))]
    drawn = drawn.at[tuple(spot)].set(least)
    longest = extent.index(max(extent))
    spot[longest] = (spot[longest] + 1) % extent[longest]
    return drawn.at[tuple(spot)].set(top_value)


def block_levels(rng, extent, split, smallest, top_value):
    gain, own = 1.0, jax.random.fold_in(rng, 6)
    for dim, parts in split:
        steps = jnp.exp(jax.random.uniform(jax.random.fold_in(own, dim), (parts,), jnp.float32, smallest / len(split), top_value / len(split)))
        gain = gain * jnp.repeat(steps, extent[dim] // parts).reshape([-1 if axis == dim else 1 for axis in range(len(extent))])
    return gain


def scatter_about(stream_key, shape, spread, limit, cuts=(), kind=jnp.bfloat16):
    array = jax.random.normal(stream_key, shape, jnp.float32) * spread
    if len(cuts) > 0:
        array = block_levels(stream_key, shape, cuts, -0.22, 0.18) * array
    return jnp.clip(array, min=-limit, max=limit).astype(kind)


def setup_inputs(seed: int = 0, part: int = 0) -> dict:
    splits = jax.random.split(jax.random.key(seed), 7)
    own_keys = jax.random.split(jax.random.fold_in(splits[6], part), 7)
    kspace = scatter_about(own_keys[0], (FRAMES, 2, COILS, KY, KX), 1.0, 6.0, ((3, 16),))
    kernel = scatter_about(splits[1], (GROUPS, KIN, 2 * COILS), KIN ** -0.5, 0.21875)
    pattern = plant(jax.random.randint(own_keys[2], (FRAMES,), 0, ALTERNATES), jax.random.fold_in(own_keys[2], 1), 0, ALTERNATES - 1).astype(jnp.int32)
    offsets = plant(jax.random.randint(splits[3], (TAPS_KX,), -2, 3), jax.random.fold_in(splits[3], 1), -2, 2).astype(jnp.int32)
    segment = plant(jax.random.randint(splits[4], (KY,), 0, ALTERNATES), jax.random.fold_in(splits[4], 1), 0, ALTERNATES - 1).astype(jnp.int32)
    temporal_basis = scatter_about(splits[5], (BASIS, FRAMES), FRAMES ** -0.5, 1.5, (), jnp.float32)
    return {"kspace": kspace, "kernel": kernel, "pattern": pattern, "offsets": offsets, "segment": segment, "temporal_basis": temporal_basis}


def reference(kspace, kernel, pattern, offsets, segment, temporal_basis):
    frame_total = kspace.shape[0]
    group_frames = frame_total // GROUPS

    def accumulate(totals, frame_item):
        frame_data, chosen, basis_column, frame_index = frame_item
        acquired = (segment == chosen)[None, None, :, None]
        zero_fill = jnp.where(acquired, frame_data, jnp.zeros_like(frame_data))
        padded = jnp.pad(zero_fill, ((0, 0), (0, 0), (1, 1), (0, 0)))
        ky_layers = []
        for ky_tap in range(TAPS_KY):
            ky_slice = padded[:, :, ky_tap:ky_tap + KY, :]
            ky_layers.append(jnp.stack([jnp.roll(ky_slice, -offsets[kx_tap], axis=3) for kx_tap in range(TAPS_KX)], axis=1))
        sources = jnp.stack(ky_layers, axis=1).reshape(KIN, KY * KX).astype(jnp.float32)
        weights = kernel[(frame_index // group_frames).astype(jnp.int32)].astype(jnp.float32)
        estimate = jnp.dot(weights.T, sources, precision=lax.Precision.HIGHEST, preferred_element_type=jnp.float32)
        estimate = estimate.reshape(2, COILS, KY, KX)
        filled = jnp.where(acquired, frame_data.astype(jnp.float32), estimate)
        return (totals + basis_column[:, None, None, None, None] * filled[None], None)
    start = jnp.zeros((BASIS, 2, COILS, KY, KX), jnp.float32)
    frame_ids = jnp.arange(frame_total, dtype=jnp.int32)
    totals, _ = lax.scan(accumulate, start, (kspace, pattern, temporal_basis.T, frame_ids))
    complex_data = totals[:, 0] + 1j * totals[:, 1]
    images = jnp.fft.ifft(complex_data, axis=2) * jnp.sqrt(jnp.float32(KY))
    stacked = jnp.stack([jnp.real(images), jnp.imag(images)], axis=1).astype(jnp.float32)
    return jnp.swapaxes(stacked, 3, 4)
```

```python
import functools

import jax
import jax.numpy as jnp
import ml_dtypes
import numpy as np
from jax import lax
from jax.experimental import pallas as pl
from jax.experimental.pallas import tpu as pltpu
from jax.sharding import PartitionSpec as P

frame_block = 4
batch = 4
sample_bound = 6.0
half_top = 60000.0
lanes = 128
sublanes = 8


def padded_2(block, sides, width):
    for axis, dim in sides:
        count = lax.axis_size(axis)
        forward = [(i, i + 1) for i in range(count - 1)]
        backward = [(target, source) for source, target in forward]
        low = lax.ppermute(
            lax.slice_in_dim(block, block.shape[dim] - width, None, axis=dim), axis, forward
        )
        high = lax.ppermute(lax.slice_in_dim(block, 0, width, axis=dim), axis, backward)
        block = jnp.concatenate([low, block, high], axis=dim)
    return block


def inverse_rows(spectra):
    row_total = spectra.shape[3]
    row_index = jnp.arange(row_total, dtype=jnp.int32)
    phase_index = row_index[:, None] * row_index[None, :] % row_total
    phase_angle = phase_index.astype(jnp.float32) * (2.0 * jnp.pi / row_total)
    cosine_table = jnp.cos(phase_angle)
    sine_table = jnp.sin(phase_angle)
    real_part = spectra[:, 0]
    imag_part = spectra[:, 1]
    high = lax.Precision.HIGHEST
    out_real = jnp.einsum("yk,mckx->mcxy", cosine_table, real_part, precision=high) - jnp.einsum(
        "yk,mckx->mcxy", sine_table, imag_part, precision=high
    )
    out_imag = jnp.einsum("yk,mckx->mcxy", sine_table, real_part, precision=high) + jnp.einsum(
        "yk,mckx->mcxy", cosine_table, imag_part, precision=high
    )
    scale = 1.0 / jnp.sqrt(jnp.float32(row_total))
    return jnp.stack([out_real, out_imag], axis=1) * scale


def plain_device(kspace, kernel, pattern, offsets, segment, temporal_basis):
    frame_total, _, coil_count, row_count, kx_count = kspace.shape
    group_count = kernel.shape[0]
    group_frames = frame_total // group_count
    row_start = lax.axis_index("ky") * row_count
    local_segment = lax.dynamic_slice_in_dim(segment, row_start, row_count)
    acquired = (local_segment[None, :] == pattern[:, None])[:, None, None, :, None]
    zero_fill = jnp.where(acquired, kspace, jnp.zeros_like(kspace))
    padded = padded_2(zero_fill, (("ky", 3),), 1)
    blocks = frame_total // frame_block
    padded_blocks = padded.reshape(blocks, frame_block, 2, coil_count, row_count + 2, kx_count)
    block_group = jnp.arange(blocks, dtype=jnp.int32) * frame_block // group_frames

    def estimate_block(block_item):
        block_data, group_index = block_item
        ky_layers = []
        for ky_tap in range(3):
            ky_slice = block_data[:, :, :, ky_tap : ky_tap + row_count, :]
            ky_layers.append(
                jnp.stack(
                    [
                        jnp.roll(ky_slice, -offsets[kx_tap], axis=4)
                        for kx_tap in range(offsets.shape[0])
                    ],
                    axis=2,
                )
            )
        sources = jnp.stack(ky_layers, axis=2).reshape(frame_block, -1, row_count * kx_count)
        weights = lax.dynamic_index_in_dim(kernel, group_index, 0, keepdims=False)
        return jnp.einsum("io,fir->for", weights, sources, preferred_element_type=jnp.float32)

    estimate = lax.map(estimate_block, (padded_blocks, block_group))
    estimate = estimate.reshape(frame_total, 2, coil_count, row_count, kx_count)
    filled = jnp.where(acquired, kspace.astype(jnp.float32), estimate)
    high = lax.Precision.HIGHEST
    coefficients = jnp.einsum("bf,fpcrx->bpcrx", temporal_basis, filled, precision=high)
    swapped = lax.all_to_all(coefficients, "ky", split_axis=4, concat_axis=3, tiled=True)
    return inverse_rows(swapped)


def row_tables(pattern, segment, temporal_basis, scale, row_count):
    frame_total = pattern.shape[0]
    row_total = segment.shape[0]
    first = lax.axis_index("ky") * row_count - 2
    rows = first + jnp.arange(row_count + 4, dtype=jnp.int32)
    inside = (rows >= 0) & (rows < row_total)
    hit = rows[:, None] == jnp.arange(row_total, dtype=jnp.int32)[None, :]
    local = jnp.sum(jnp.where(hit, segment[None, :], 0), axis=1)
    taken = (local[:, None] == pattern[None, :]) & inside[:, None]
    missing = jnp.where(taken | ~inside[:, None], 0.0, 1.0)
    source = taken[1:-1]
    frame = jnp.arange(frame_total, dtype=jnp.int32)
    before = (frame[None, :] < frame[:, None]).astype(jnp.int32)
    rank = jnp.sum(source.astype(jnp.int32)[:, None, :] * before[None], axis=2)
    count = jnp.sum(source.astype(jnp.int32), axis=1)
    place = (rank[:, None, :] == frame[None, :, None]) & source[:, None, :]
    order = jnp.sum(jnp.where(place, frame[None, None, :], 0), axis=2)
    held = jnp.where(source, 1.0, 0.0)
    own = jnp.where(jnp.arange(row_count + 2) % (row_count + 1) == 0, 0.0, 1.0)[:, None]
    masks = jnp.stack(
        [held * own, held * missing[2:], held * missing[:-2], held * missing[1:-1] * own], axis=1
    )
    middle = jnp.sum(masks[:, 3], axis=1).astype(jnp.int32)
    scaled = temporal_basis * scale[:, None]
    picked = jnp.where(place[:, :, None, None, :], masks[:, None, :, None, :], 0.0)
    weights = jnp.sum(picked * scaled[None, None, None], axis=4)
    return order.reshape(-1), count, middle, weights.reshape(-1)


def fill_kernel(
    row_count,
    order_ref,
    count_ref,
    middle_ref,
    weight_ref,
    offset_ref,
    block_ref,
    low_ref,
    high_ref,
    tap_ref,
    out_ref,
    samples,
    source,
    product,
    totals,
):
    frame_total, halves, _, _ = samples.shape
    parts, kx_count = source.shape[1:]
    basis_count = totals.shape[1]
    group_frames = frame_total // tap_ref.shape[0]
    taps = offset_ref.shape[0]
    step = pl.program_id(0)

    @pl.when(step < frame_total)
    def _():
        values = block_ref[0].astype(jnp.float32).reshape(parts * row_count, kx_count)
        for half in range(halves):
            samples[step, half] = values[:, half * lanes : (half + 1) * lanes]

    @pl.when(step == 0)
    def _():
        totals[...] = jnp.zeros_like(totals)

    @pl.when(step >= frame_total)
    def _():
        slot = step - frame_total
        row = slot - 1
        here = lax.rem(slot, 3)
        after = lax.rem(slot + 1, 3)
        back = lax.rem(slot + 2, 3)
        totals[after] = jnp.zeros_like(totals[after])

        def load(entry, position):
            frame = order_ref[slot * frame_total + position]

            @pl.when(slot == 0)
            def _():
                source[entry] = low_ref[frame].astype(jnp.float32)

            @pl.when(slot == row_count + 1)
            def _():
                source[entry] = high_ref[frame].astype(jnp.float32)

            @pl.when((slot > 0) & (slot <= row_count))
            def _():
                for half in range(halves):
                    source[entry, :, half * lanes : (half + 1) * lanes] = samples[
                        frame, half, pl.ds(row, parts, stride=row_count), :
                    ]

            return frame // group_frames

        def shifted(entry):
            narrow = source[entry].astype(jnp.bfloat16)
            return jnp.concatenate(
                [
                    pltpu.roll(narrow, lax.rem(kx_count - offset_ref[tap], kx_count), axis=1)
                    for tap in range(taps)
                ],
                axis=0,
            )

        def add(target, kind, entries, base):
            scalars = [
                [
                    weight_ref[((slot * frame_total + base + e) * 4 + kind) * basis_count + v]
                    for v in range(basis_count)
                ]
                for e in range(len(entries))
            ]
            for start in range(0, parts, sublanes):
                pieces = [read(start) for read in entries]
                for v in range(basis_count):
                    total = totals[target, v, start : start + sublanes, :]
                    for e, piece in enumerate(pieces):
                        total = total + scalars[e][v] * piece
                    totals[target, v, start : start + sublanes, :] = total

        def reader(ref, entry, offset):
            return lambda start: ref[entry, offset + start : offset + start + sublanes, :]

        def body(index, carry):
            base = index * batch
            for e in range(batch):
                group = load(e, base + e)
                product[e] = jnp.dot(
                    tap_ref[group, : 2 * parts],
                    shifted(e),
                    preferred_element_type=jnp.float32,
                )
            add(here, 0, [reader(source, e, 0) for e in range(batch)], base)
            add(after, 1, [reader(product, e, 0) for e in range(batch)], base)
            add(back, 2, [reader(product, e, parts) for e in range(batch)], base)
            return carry

        lax.fori_loop(0, (count_ref[slot] + batch - 1) // batch, body, 0)

        def middle(index, carry):
            group = load(0, index)
            product[0, :parts] = jnp.dot(
                tap_ref[group, 2 * parts :], shifted(0), preferred_element_type=jnp.float32
            )
            add(here, 3, [reader(product, 0, 0)], index)
            return carry

        lax.fori_loop(0, jnp.where(middle_ref[slot] > 0, count_ref[slot], 0), middle, 0)

        @pl.when(slot >= 2)
        def _():
            devices, _, stored, _ = out_ref.shape
            inner = stored // row_count
            packed = lanes // parts
            for v in range(basis_count):
                turned = totals[back, v].T.reshape(devices, packed, inner, parts)
                joined = jnp.concatenate([turned[:, j] for j in range(packed)], axis=-1)
                for d in range(devices):
                    out_ref[d, v, pl.ds(row - 1, inner, stride=row_count), :] = joined[d]


def image_kernel(row_count, coil_count, inverse_ref, block_ref, table_ref, out_ref, held):
    devices, _, stored, _ = block_ref.shape
    halves, part_count, length, _ = held.shape
    inner = stored // row_count
    columns = length // coil_count
    parts = part_count * coil_count
    row_total = devices * row_count
    scale = inverse_ref[pl.program_id(0)]
    for i in range(inner):
        turned = block_ref[:, 0, i * row_count : (i + 1) * row_count, :].reshape(row_total, lanes).T
        for j in range(lanes // parts):
            for p in range(part_count):
                start = j * parts + p * coil_count
                for half in range(halves):
                    held[half, p, pl.ds(j * inner + i, coil_count, stride=columns), :] = turned[
                        start : start + coil_count, half * lanes : (half + 1) * lanes
                    ]
    for start in range(0, length, lanes):
        left = jnp.concatenate(
            [
                held[half, p, start : start + lanes, :]
                for p in range(part_count)
                for half in range(halves)
            ],
            axis=1,
        )
        coarse = left.astype(jnp.bfloat16)
        fine = (left - coarse.astype(jnp.float32)).astype(jnp.bfloat16)
        result = jnp.dot(coarse, table_ref[0], preferred_element_type=jnp.float32)
        result = result + jnp.dot(coarse, table_ref[1], preferred_element_type=jnp.float32)
        result = result + jnp.dot(fine, table_ref[0], preferred_element_type=jnp.float32)
        result = result * scale
        for p in range(part_count):
            out_ref[0, p, start : start + lanes, :] = result[:, p * row_total : (p + 1) * row_total]


def inverse_table(row_total):
    index = np.arange(row_total)
    angle = (index[:, None] * index[None, :] % row_total) * (2.0 * np.pi / row_total)
    cosine = np.cos(angle) / np.sqrt(row_total)
    sine = np.sin(angle) / np.sqrt(row_total)
    full = np.block([[cosine, sine], [-sine, cosine]]).astype(np.float32)
    coarse = full.astype(ml_dtypes.bfloat16)
    fine = (full - coarse.astype(np.float32)).astype(ml_dtypes.bfloat16)
    return np.stack([coarse, fine])


def on_device(kspace, kernel, pattern, offsets, segment, temporal_basis):
    frame_total, part_count, coil_count, row_count, kx_count = kspace.shape
    devices = lax.axis_size("ky")
    columns = kx_count // devices
    parts = part_count * coil_count
    row_total = row_count * devices
    fits = (
        row_count % (2 * sublanes) == 0
        and lanes % parts == 0
        and columns == sublanes * (lanes // parts)
        and kx_count % lanes == 0
        and row_total % lanes == 0
        and frame_total % batch == 0
    )
    if not fits:
        return plain_device(kspace, kernel, pattern, offsets, segment, temporal_basis)

    basis_count = temporal_basis.shape[0]
    group_count = kernel.shape[0]
    tap_count = offsets.shape[0]
    inner = sublanes
    stored = inner * row_count
    halves = kx_count // lanes

    forward = [(i, i + 1) for i in range(devices - 1)]
    backward = [(i + 1, i) for i in range(devices - 1)]
    edge_shape = (frame_total, parts, kx_count)
    low = lax.ppermute(kspace[:, :, :, -1, :].reshape(edge_shape), "ky", forward)
    high = lax.ppermute(kspace[:, :, :, 0, :].reshape(edge_shape), "ky", backward)

    strength = jnp.max(jnp.sum(jnp.abs(kernel.astype(jnp.float32)), axis=1))
    bound = sample_bound * jnp.sum(jnp.abs(temporal_basis), axis=1) * jnp.maximum(strength, 1.0)
    power = jnp.clip(jnp.floor(jnp.log2(half_top / jnp.maximum(bound, 1e-30))), -60.0, 60.0)
    scale = jnp.exp2(power)
    order, count, middle, weights = row_tables(
        pattern, segment, temporal_basis, scale, row_count
    )
    tap_rows = kernel.reshape(group_count, part_count, 3, tap_count, coil_count, parts)
    tap_rows = tap_rows.transpose(0, 2, 5, 3, 1, 4).reshape(
        group_count, 3, parts, tap_count * parts
    )
    tap_rows = jnp.concatenate([tap_rows[:, 0], tap_rows[:, 2], tap_rows[:, 1]], axis=1)

    scalar = pl.BlockSpec(memory_space=pltpu.SMEM)
    edge = pl.BlockSpec(edge_shape, lambda t: (0, 0, 0))
    payload = pl.pallas_call(
        functools.partial(fill_kernel, row_count),
        grid=(frame_total + row_count + 2,),
        in_specs=[
            scalar,
            scalar,
            scalar,
            scalar,
            scalar,
            pl.BlockSpec(
                (1, parts, row_count, kx_count),
                lambda t: (jnp.minimum(t, frame_total - 1), 0, 0, 0),
            ),
            edge,
            edge,
            pl.BlockSpec(tap_rows.shape, lambda t: (0, 0, 0)),
        ],
        out_specs=pl.BlockSpec((devices, basis_count, stored, lanes), lambda t: (0, 0, 0, 0)),
        out_shape=jax.ShapeDtypeStruct((devices, basis_count, stored, lanes), jnp.float32),
        scratch_shapes=[
            pltpu.VMEM((frame_total, halves, parts * row_count, lanes), jnp.float32),
            pltpu.VMEM((batch, parts, kx_count), jnp.float32),
            pltpu.VMEM((batch, 2 * parts, kx_count), jnp.float32),
            pltpu.VMEM((3, basis_count, parts, kx_count), jnp.float32),
        ],
        name="fill",
    )(
        order,
        count,
        middle,
        weights,
        offsets,
        kspace.reshape(frame_total, parts, row_count, kx_count),
        low,
        high,
        tap_rows,
    )
    swapped = lax.all_to_all(
        payload.astype(jnp.float16), "ky", split_axis=0, concat_axis=0, tiled=True
    ).astype(jnp.float32)

    table = jnp.asarray(inverse_table(row_total))
    length = coil_count * columns
    images = pl.pallas_call(
        functools.partial(image_kernel, row_count, coil_count),
        grid=(basis_count,),
        in_specs=[
            scalar,
            pl.BlockSpec((devices, 1, stored, lanes), lambda v: (0, v, 0, 0)),
            pl.BlockSpec(table.shape, lambda v: (0, 0, 0)),
        ],
        out_specs=pl.BlockSpec((1, part_count, length, row_total), lambda v: (v, 0, 0, 0)),
        out_shape=jax.ShapeDtypeStruct(
            (basis_count, part_count, length, row_total), jnp.float32
        ),
        scratch_shapes=[
            pltpu.VMEM((row_total // lanes, part_count, length, lanes), jnp.float32)
        ],
        name="image",
    )(1.0 / scale, swapped, table)
    return images.reshape(basis_count, part_count, coil_count, columns, row_total)


def solution(mesh):
    return jax.shard_map(
        on_device,
        mesh=mesh,
        in_specs=(P("study", None, None, "ky", None), P(), P("study"), P(), P(), P()),
        out_specs=P("study", None, None, "ky", None),
        check_vma=False,
    )
```

```python
import functools

import jax
import jax.numpy as jnp
import ml_dtypes
import numpy as np
from jax import lax
from jax.experimental import pallas as pl
from jax.experimental.pallas import tpu as pltpu
from jax.sharding import PartitionSpec as P

frame_block = 4
batch = 4
together = 2
pair = 2
sample_bound = 6.0
half_top = 60000.0
lanes = 128
sublanes = 8


def padded_2(block, sides, width):
    for axis, dim in sides:
        count = lax.axis_size(axis)
        forward = [(i, i + 1) for i in range(count - 1)]
        backward = [(target, source) for source, target in forward]
        low = lax.ppermute(
            lax.slice_in_dim(block, block.shape[dim] - width, None, axis=dim), axis, forward
        )
        high = lax.ppermute(lax.slice_in_dim(block, 0, width, axis=dim), axis, backward)
        block = jnp.concatenate([low, block, high], axis=dim)
    return block


def inverse_rows(spectra):
    row_total = spectra.shape[3]
    row_index = jnp.arange(row_total, dtype=jnp.int32)
    phase_index = row_index[:, None] * row_index[None, :] % row_total
    phase_angle = phase_index.astype(jnp.float32) * (2.0 * jnp.pi / row_total)
    cosine_table = jnp.cos(phase_angle)
    sine_table = jnp.sin(phase_angle)
    real_part = spectra[:, 0]
    imag_part = spectra[:, 1]
    high = lax.Precision.HIGHEST
    out_real = jnp.einsum("yk,mckx->mcxy", cosine_table, real_part, precision=high) - jnp.einsum(
        "yk,mckx->mcxy", sine_table, imag_part, precision=high
    )
    out_imag = jnp.einsum("yk,mckx->mcxy", sine_table, real_part, precision=high) + jnp.einsum(
        "yk,mckx->mcxy", cosine_table, imag_part, precision=high
    )
    scale = 1.0 / jnp.sqrt(jnp.float32(row_total))
    return jnp.stack([out_real, out_imag], axis=1) * scale


def plain_device(kspace, kernel, pattern, offsets, segment, temporal_basis):
    frame_total, _, coil_count, row_count, kx_count = kspace.shape
    group_count = kernel.shape[0]
    group_frames = frame_total // group_count
    row_start = lax.axis_index("ky") * row_count
    local_segment = lax.dynamic_slice_in_dim(segment, row_start, row_count)
    acquired = (local_segment[None, :] == pattern[:, None])[:, None, None, :, None]
    zero_fill = jnp.where(acquired, kspace, jnp.zeros_like(kspace))
    padded = padded_2(zero_fill, (("ky", 3),), 1)
    blocks = frame_total // frame_block
    padded_blocks = padded.reshape(blocks, frame_block, 2, coil_count, row_count + 2, kx_count)
    block_group = jnp.arange(blocks, dtype=jnp.int32) * frame_block // group_frames

    def estimate_block(block_item):
        block_data, group_index = block_item
        ky_layers = []
        for ky_tap in range(3):
            ky_slice = block_data[:, :, :, ky_tap : ky_tap + row_count, :]
            ky_layers.append(
                jnp.stack(
                    [
                        jnp.roll(ky_slice, -offsets[kx_tap], axis=4)
                        for kx_tap in range(offsets.shape[0])
                    ],
                    axis=2,
                )
            )
        sources = jnp.stack(ky_layers, axis=2).reshape(frame_block, -1, row_count * kx_count)
        weights = lax.dynamic_index_in_dim(kernel, group_index, 0, keepdims=False)
        return jnp.einsum("io,fir->for", weights, sources, preferred_element_type=jnp.float32)

    estimate = lax.map(estimate_block, (padded_blocks, block_group))
    estimate = estimate.reshape(frame_total, 2, coil_count, row_count, kx_count)
    filled = jnp.where(acquired, kspace.astype(jnp.float32), estimate)
    high = lax.Precision.HIGHEST
    coefficients = jnp.einsum("bf,fpcrx->bpcrx", temporal_basis, filled, precision=high)
    swapped = lax.all_to_all(coefficients, "ky", split_axis=4, concat_axis=3, tiled=True)
    return inverse_rows(swapped)


class Filler:

    def __init__(self, refs, scratch, parts, kx_count):
        self.place, self.pattern, self.segment, self.offset, self.basis, self.kernel = refs
        self.source, self.product, self.totals, self.taps, self.order, self.count, self.scale = (
            scratch
        )
        self.parts = parts
        self.kx_count = kx_count
        self.frame_total = self.pattern.shape[0]
        self.row_total = self.segment.shape[0]
        self.basis_count = self.basis.shape[0]
        self.group_count = self.kernel.shape[0]
        self.group_frames = self.frame_total // self.group_count
        self.tap_count = self.offset.shape[0]
        self.coil_count = parts // 2

    def row_of(self, local):
        row = self.place[0] + local
        inside = (row >= 0) & (row < self.row_total)
        return self.segment[jnp.clip(row, 0, self.row_total - 1)], inside

    def prepare(self, shape):
        self.totals[...] = jnp.zeros_like(self.totals)
        width = self.tap_count * self.coil_count
        strength = jnp.float32(1.0)
        for group in range(self.group_count):
            for tap in range(3):
                joined = jnp.concatenate(
                    [
                        self.kernel[group, :, (p * 3 + tap) * width : (p * 3 + tap + 1) * width]
                        for p in range(2)
                    ],
                    axis=1,
                )
                self.taps[group, tap * self.parts : (tap + 1) * self.parts, :] = joined
            reach = jnp.sum(jnp.abs(self.kernel[group].astype(jnp.float32)), axis=1, keepdims=True)
            strength = jnp.maximum(strength, jnp.max(reach))
        extent = jnp.float32(0.0)
        for v in range(self.basis_count):
            extent_v = jnp.float32(0.0)
            for frame in range(self.frame_total):
                extent_v = extent_v + jnp.abs(self.basis[v, frame])
            extent = jnp.maximum(extent, extent_v)
        bound = jnp.maximum(sample_bound * extent * strength, 1e-30)
        scale = half_top / jnp.full(shape, bound, jnp.float32)
        self.scale[0] = jnp.max(scale)
        return 1.0 / scale

    def listing(self, slot, local):
        value, inside = self.row_of(local)
        filled = jnp.int32(0)
        doubled = jnp.int32(0)
        again, _ = self.row_of(local)
        for frame in range(self.frame_total):
            taken = (value == self.pattern[frame]) & inside
            self.order[slot * self.frame_total + filled] = frame
            filled = filled + taken.astype(jnp.int32)
            doubled = doubled + (taken & (again != self.pattern[frame])).astype(jnp.int32)
        self.count[2 * slot] = filled
        self.count[2 * slot + 1] = doubled

    def shifted(self, entry):
        narrow = self.source[entry].astype(jnp.bfloat16)
        shifts = [
            lax.rem(self.kx_count - self.offset[tap], self.kx_count)
            for tap in range(self.tap_count)
        ]
        return jnp.concatenate(
            [
                pltpu.roll(narrow[p * self.coil_count : (p + 1) * self.coil_count], shift, axis=1)
                for p in range(2)
                for shift in shifts
            ],
            axis=0,
        )

    def add(self, target, weights, entries):
        for start in range(0, self.parts, sublanes):
            pieces = [
                ref[entry, offset + start : offset + start + sublanes, :]
                for ref, entry, offset in entries
            ]
            for v in range(self.basis_count):
                total = self.totals[target, v, start : start + sublanes, :]
                for weight, piece in zip(weights, pieces):
                    total = total + weight[v] * piece
                self.totals[target, v, start : start + sublanes, :] = total

    def multiply(self, entry, group, tap, offset):
        self.product[entry, offset : offset + self.parts] = jnp.dot(
            self.taps[group, tap * self.parts : (tap + 1) * self.parts],
            self.shifted(entry),
            preferred_element_type=jnp.float32,
        )

    def row(self, slot, local, fetch, targets):
        listed = self.count[2 * slot]
        parts = self.parts
        neighbours = [self.row_of(local + 1 - tap) for tap in range(3)]

        def load(entry, position):
            frame = self.order[slot * self.frame_total + jnp.minimum(position, listed - 1)]
            fetch(entry, frame)
            scale = jnp.where(position < listed, self.scale[0], 0.0)
            direct = [self.basis[v, frame] * scale for v in range(self.basis_count)]
            wanted = self.pattern[frame]
            masked = [
                [jnp.where(inside & (value != wanted), weight, 0.0) for weight in direct]
                for value, inside in neighbours
            ]
            return frame // self.group_frames, direct, masked

        def batch_at(base, size):
            each = range(size)
            loaded = [load(e, base + e) for e in each]
            sides = [tap for tap in (0, 2) if targets[tap] is not None]
            for e in each:
                for tap in sides:
                    self.multiply(e, loaded[e][0], tap, tap // 2 * parts)
            if targets[1] is not None:
                self.add(
                    targets[1], [loaded[e][1] for e in each], [(self.source, e, 0) for e in each]
                )
            for tap in sides:
                self.add(
                    targets[tap],
                    [loaded[e][2][tap] for e in each],
                    [(self.product, e, tap // 2 * parts) for e in each],
                )

        def full(index, carry):
            batch_at(index * batch, batch)
            return carry

        whole = listed // batch
        rest = listed - whole * batch
        large = (rest > batch // 2).astype(jnp.int32)
        lax.fori_loop(0, whole + large, full, 0)

        @pl.when((rest > 0) & (large == 0))
        def _():
            batch_at(whole * batch, batch // 2)

        def centre(index, carry):
            group, _, masked = load(0, index)
            self.multiply(0, group, 1, 0)
            self.add(targets[1], [masked[1]], [(self.product, 0, 0)])
            return carry

        if targets[1] is not None:
            lax.fori_loop(0, jnp.where(self.count[2 * slot + 1] > 0, listed, 0), centre, 0)


def fill_kernel(
    row_count,
    place_ref,
    pattern_ref,
    segment_ref,
    offset_ref,
    basis_ref,
    block_ref,
    kernel_ref,
    out_ref,
    inverse_ref,
    samples,
    *scratch,
):
    _, halves, _, _ = samples.shape
    together, parts, _, kx_count = block_ref.shape
    refs = (place_ref, pattern_ref, segment_ref, offset_ref, basis_ref, kernel_ref)
    filler = Filler(refs, scratch, parts, kx_count)
    step = pl.program_id(0)

    for t in range(together):
        values = block_ref[t].astype(jnp.float32).reshape(parts * row_count, kx_count)
        for half in range(halves):
            samples[step * together + t, half] = values[:, half * lanes : (half + 1) * lanes]

    @pl.when(step == 0)
    def _():
        inverse_ref[...] = filler.prepare(inverse_ref.shape)

        def listing(row, carry):
            filler.listing(row, row)
            return carry

        lax.fori_loop(0, row_count, listing, 0)

    def rows(row, carry):
        def fetch(entry, frame):
            for half in range(halves):
                filler.source[entry, :, half * lanes : (half + 1) * lanes] = samples[
                    frame, half, pl.ds(row, parts, stride=row_count), :
                ]

        filler.row(row, row, fetch, (row + 2, row + 1, row))
        return carry

    def pack(index, carry):
        devices, basis_count, stored, _ = out_ref.shape
        pitch = row_count // pair
        columns = stored // pitch
        for v in range(basis_count):
            turned = jnp.concatenate(
                [filler.totals[pair * index + 1 + j, v] for j in range(pair)], axis=0
            ).T
            for d in range(devices):
                out_ref[d, v, pl.ds(index, columns, stride=pitch), :] = turned[
                    d * columns : (d + 1) * columns
                ]
        return carry

    @pl.when(step == pl.num_programs(0) - 1)
    def _():
        lax.fori_loop(0, row_count, rows, 0)
        lax.fori_loop(0, row_count // pair, pack, 0)


def edge_kernel(
    row_count,
    place_ref,
    pattern_ref,
    segment_ref,
    offset_ref,
    basis_ref,
    low_ref,
    high_ref,
    kernel_ref,
    out_ref,
    *scratch,
):
    _, parts, kx_count = low_ref.shape
    refs = (place_ref, pattern_ref, segment_ref, offset_ref, basis_ref, kernel_ref)
    filler = Filler(refs, scratch, parts, kx_count)
    filler.prepare((sublanes, lanes))
    sides = ((-1, low_ref, (0, None, None)), (row_count, high_ref, (None, None, 1)))
    for slot, (local, ref, targets) in enumerate(sides):
        filler.listing(slot, local)

        def fetch(entry, frame):
            filler.source[entry] = ref[frame].astype(jnp.float32)

        filler.row(slot, local, fetch, targets)
    devices, basis_count, columns, _ = out_ref.shape
    for v in range(basis_count):
        turned = jnp.concatenate([filler.totals[0, v], filler.totals[1, v]], axis=0).T
        for d in range(devices):
            out_ref[d, v] = turned[d * columns : (d + 1) * columns]


def image_kernel(row_count, coil_count, inverse_ref, block_ref, table_ref, out_ref, held):
    devices, _, stored, _ = block_ref.shape
    pair, part_count, length, width = held.shape
    pitch = row_count // pair
    columns = stored // pitch
    parts = part_count * coil_count
    row_total = devices * row_count
    scale = inverse_ref[0:1, 0:1]
    for x in range(columns):
        turned = block_ref[:, 0, x * pitch : (x + 1) * pitch, :].reshape(width, lanes).T
        for j in range(pair):
            for p in range(part_count):
                start = j * parts + p * coil_count
                held[j, p, pl.ds(x, coil_count, stride=columns), :] = turned[
                    start : start + coil_count
                ]
    for start in range(0, length, lanes):
        left = jnp.concatenate(
            [
                held[j, p, start : start + lanes, :]
                for p in range(part_count)
                for j in range(pair)
            ],
            axis=1,
        )
        coarse = left.astype(jnp.bfloat16)
        fine = (left - coarse.astype(jnp.float32)).astype(jnp.bfloat16)
        result = jnp.dot(coarse, table_ref[0], preferred_element_type=jnp.float32)
        result = result + jnp.dot(coarse, table_ref[1], preferred_element_type=jnp.float32)
        result = result + jnp.dot(fine, table_ref[0], preferred_element_type=jnp.float32)
        result = result * scale
        for p in range(part_count):
            out_ref[0, p, start : start + lanes, :] = result[:, p * row_total : (p + 1) * row_total]


def inverse_table(row_total, pair):
    row = np.arange(row_total).reshape(-1, pair).T.reshape(-1)
    index = np.arange(row_total)
    angle = (row[:, None] * index[None, :] % row_total) * (2.0 * np.pi / row_total)
    cosine = np.cos(angle) / np.sqrt(row_total)
    sine = np.sin(angle) / np.sqrt(row_total)
    full = np.block([[cosine, sine], [-sine, cosine]]).astype(np.float32)
    coarse = full.astype(ml_dtypes.bfloat16)
    fine = (full - coarse.astype(np.float32)).astype(ml_dtypes.bfloat16)
    return np.stack([coarse, fine])


def on_device(kspace, kernel, pattern, offsets, segment, temporal_basis):
    frame_total, part_count, coil_count, row_count, kx_count = kspace.shape
    devices = lax.axis_size("ky")
    columns = kx_count // devices
    parts = part_count * coil_count
    row_total = row_count * devices
    tap_count = offsets.shape[0]
    fits = (
        2 * parts == lanes
        and row_count == 2 * sublanes
        and columns % sublanes == 0
        and row_total == 2 * lanes
        and kx_count % lanes == 0
        and tap_count * coil_count == lanes
        and frame_total % together == 0
    )
    if not fits:
        return plain_device(kspace, kernel, pattern, offsets, segment, temporal_basis)

    basis_count = temporal_basis.shape[0]
    group_count = kernel.shape[0]
    stored = columns * row_count // pair
    halves = kx_count // lanes

    forward = [(i, i + 1) for i in range(devices - 1)]
    backward = [(i + 1, i) for i in range(devices - 1)]
    edge_shape = (frame_total, parts, kx_count)
    low = lax.ppermute(kspace[:, :, :, -1, :].reshape(edge_shape), "ky", forward)
    high = lax.ppermute(kspace[:, :, :, 0, :].reshape(edge_shape), "ky", backward)

    place = (lax.axis_index("ky") * row_count).astype(jnp.int32).reshape(1)
    kernel_rows = kernel.transpose(0, 2, 1)
    fill_work = 4 * frame_total * row_count * kx_count * kernel.shape[1] * parts

    scalar = pl.BlockSpec(memory_space=pltpu.SMEM)

    def scratch(rows, slots):
        return [
            pltpu.VMEM((batch, parts, kx_count), jnp.float32),
            pltpu.VMEM((batch, 2 * parts, kx_count), jnp.float32),
            pltpu.VMEM((rows, basis_count, parts, kx_count), jnp.float32),
            pltpu.VMEM((group_count, 3 * parts, tap_count * parts), jnp.bfloat16),
            pltpu.SMEM((slots * frame_total + 1,), jnp.int32),
            pltpu.SMEM((2 * slots,), jnp.int32),
            pltpu.SMEM((1,), jnp.float32),
        ]

    scalars = (place, pattern, segment, offsets, temporal_basis)
    payload, inverse = pl.pallas_call(
        functools.partial(fill_kernel, row_count),
        grid=(frame_total // together,),
        in_specs=[scalar] * len(scalars)
        + [
            pl.BlockSpec((together, parts, row_count, kx_count), lambda t: (t, 0, 0, 0)),
            pl.BlockSpec(kernel_rows.shape, lambda t: (0, 0, 0)),
        ],
        out_specs=[
            pl.BlockSpec((devices, basis_count, stored, lanes), lambda t: (0, 0, 0, 0)),
            pl.BlockSpec((sublanes, lanes), lambda t: (0, 0)),
        ],
        out_shape=[
            jax.ShapeDtypeStruct((devices, basis_count, stored, lanes), jnp.float32),
            jax.ShapeDtypeStruct((sublanes, lanes), jnp.float32),
        ],
        scratch_shapes=[
            pltpu.VMEM((frame_total, halves, parts * row_count, lanes), jnp.float32)
        ]
        + scratch(row_count + 2, row_count),
        cost_estimate=pl.CostEstimate(flops=fill_work, bytes_accessed=0, transcendentals=0),
        name="fill",
    )(*scalars, kspace.reshape(frame_total, parts, row_count, kx_count), kernel_rows)
    whole = pl.BlockSpec(memory_space=pltpu.VMEM)
    edges = pl.pallas_call(
        functools.partial(edge_kernel, row_count),
        in_specs=[scalar] * len(scalars) + [whole] * 3,
        out_specs=whole,
        out_shape=jax.ShapeDtypeStruct((devices, basis_count, columns, lanes), jnp.float32),
        scratch_shapes=scratch(2, 2),
        name="edge",
    )(*scalars, low, high, kernel_rows)
    spread = payload.reshape(devices, basis_count, columns, row_count // pair, lanes)
    place_in = lax.broadcasted_iota(jnp.int32, spread.shape, 3)
    lane = lax.broadcasted_iota(jnp.int32, spread.shape, 4)
    outer = jnp.where(lane < parts, 0, row_count // pair - 1) == place_in
    spread = spread + jnp.where(outer, edges[:, :, :, None, :], 0.0)
    payload = spread.astype(jnp.float16).reshape(devices, basis_count, stored, lanes)
    swapped = lax.all_to_all(
        payload, "ky", split_axis=0, concat_axis=0, tiled=True
    ).astype(jnp.float32)

    table = jnp.asarray(inverse_table(row_total, pair))
    length = coil_count * columns
    images = pl.pallas_call(
        functools.partial(image_kernel, row_count, coil_count),
        grid=(basis_count,),
        in_specs=[
            pl.BlockSpec((sublanes, lanes), lambda v: (0, 0)),
            pl.BlockSpec((devices, 1, stored, lanes), lambda v: (0, v, 0, 0)),
            pl.BlockSpec(table.shape, lambda v: (0, 0, 0)),
        ],
        out_specs=pl.BlockSpec((1, part_count, length, row_total), lambda v: (v, 0, 0, 0)),
        out_shape=jax.ShapeDtypeStruct(
            (basis_count, part_count, length, row_total), jnp.float32
        ),
        scratch_shapes=[
            pltpu.VMEM((pair, part_count, length, row_total // pair), jnp.float32)
        ],
        name="image",
    )(inverse, swapped, table)
    return images.reshape(basis_count, part_count, coil_count, columns, row_total)


def solution(mesh):
    return jax.shard_map(
        on_device,
        mesh=mesh,
        in_specs=(P("study", None, None, "ky", None), P(), P("study"), P(), P(), P()),
        out_specs=P("study", None, None, "ky", None),
        check_vma=False,
    )
```

```python
import functools

import jax
import jax.numpy as jnp
import ml_dtypes
import numpy as np
from jax import lax
from jax.experimental import pallas as pl
from jax.experimental.pallas import tpu as pltpu
from jax.sharding import PartitionSpec as P


frame_block = 4
batch = 4
together = 8
sample_bound = 6.0
half_top = 60000.0
lanes = 128
sublanes = 8


def padded_2(block, sides, width):
    for axis, dim in sides:
        count = lax.axis_size(axis)
        forward = [(i, i + 1) for i in range(count - 1)]
        backward = [(target, source) for source, target in forward]
        low = lax.ppermute(
            lax.slice_in_dim(block, block.shape[dim] - width, None, axis=dim), axis, forward
        )
        high = lax.ppermute(lax.slice_in_dim(block, 0, width, axis=dim), axis, backward)
        block = jnp.concatenate([low, block, high], axis=dim)
    return block


def inverse_rows(spectra):
    row_total = spectra.shape[3]
    row_index = jnp.arange(row_total, dtype=jnp.int32)
    phase_index = row_index[:, None] * row_index[None, :] % row_total
    phase_angle = phase_index.astype(jnp.float32) * (2.0 * jnp.pi / row_total)
    cosine_table = jnp.cos(phase_angle)
    sine_table = jnp.sin(phase_angle)
    real_part = spectra[:, 0]
    imag_part = spectra[:, 1]
    high = lax.Precision.HIGHEST
    out_real = jnp.einsum("yk,mckx->mcxy", cosine_table, real_part, precision=high) - jnp.einsum(
        "yk,mckx->mcxy", sine_table, imag_part, precision=high
    )
    out_imag = jnp.einsum("yk,mckx->mcxy", sine_table, real_part, precision=high) + jnp.einsum(
        "yk,mckx->mcxy", cosine_table, imag_part, precision=high
    )
    scale = 1.0 / jnp.sqrt(jnp.float32(row_total))
    return jnp.stack([out_real, out_imag], axis=1) * scale


def plain_device(kspace, kernel, pattern, offsets, segment, temporal_basis):
    frame_total, _, coil_count, row_count, kx_count = kspace.shape
    group_count = kernel.shape[0]
    group_frames = frame_total // group_count
    row_start = lax.axis_index("ky") * row_count
    local_segment = lax.dynamic_slice_in_dim(segment, row_start, row_count)
    acquired = (local_segment[None, :] == pattern[:, None])[:, None, None, :, None]
    zero_fill = jnp.where(acquired, kspace, jnp.zeros_like(kspace))
    padded = padded_2(zero_fill, (("ky", 3),), 1)
    blocks = frame_total // frame_block
    padded_blocks = padded.reshape(blocks, frame_block, 2, coil_count, row_count + 2, kx_count)
    block_group = jnp.arange(blocks, dtype=jnp.int32) * frame_block // group_frames

    def estimate_block(block_item):
        block_data, group_index = block_item
        ky_layers = []
        for ky_tap in range(3):
            ky_slice = block_data[:, :, :, ky_tap : ky_tap + row_count, :]
            ky_layers.append(
                jnp.stack(
                    [
                        jnp.roll(ky_slice, -offsets[kx_tap], axis=4)
                        for kx_tap in range(offsets.shape[0])
                    ],
                    axis=2,
                )
            )
        sources = jnp.stack(ky_layers, axis=2).reshape(frame_block, -1, row_count * kx_count)
        weights = lax.dynamic_index_in_dim(kernel, group_index, 0, keepdims=False)
        return jnp.einsum("io,fir->for", weights, sources, preferred_element_type=jnp.float32)

    estimate = lax.map(estimate_block, (padded_blocks, block_group))
    estimate = estimate.reshape(frame_total, 2, coil_count, row_count, kx_count)
    filled = jnp.where(acquired, kspace.astype(jnp.float32), estimate)
    high = lax.Precision.HIGHEST
    coefficients = jnp.einsum("bf,fpcrx->bpcrx", temporal_basis, filled, precision=high)
    swapped = lax.all_to_all(coefficients, "ky", split_axis=4, concat_axis=3, tiled=True)
    return inverse_rows(swapped)


class Filler:

    def __init__(self, refs, scratch, parts, kx_count):
        self.place, self.pattern, self.segment, self.offset, self.basis, self.kernel = refs
        self.source, self.product, self.totals, self.taps, self.order, self.count, self.scale = (
            scratch
        )
        self.parts = parts
        self.kx_count = kx_count
        self.frame_total = self.pattern.shape[0]
        self.row_total = self.segment.shape[0]
        self.basis_count = self.basis.shape[0]
        self.group_count = self.kernel.shape[0]
        self.group_frames = self.frame_total // self.group_count
        self.tap_count = self.offset.shape[0]
        self.coil_count = parts // 2

    def row_of(self, local):
        row = self.place[0] + local
        inside = (row >= 0) & (row < self.row_total)
        return self.segment[jnp.clip(row, 0, self.row_total - 1)], inside

    def prepare(self, shape):
        self.totals[...] = jnp.zeros_like(self.totals)
        width = self.tap_count * self.coil_count
        strength = jnp.float32(1.0)
        for group in range(self.group_count):
            for tap in range(3):
                joined = jnp.concatenate(
                    [
                        self.kernel[group, :, (p * 3 + tap) * width : (p * 3 + tap + 1) * width]
                        for p in range(2)
                    ],
                    axis=1,
                )
                self.taps[group, tap * self.parts : (tap + 1) * self.parts, :] = joined
            reach = jnp.sum(jnp.abs(self.kernel[group].astype(jnp.float32)), axis=1, keepdims=True)
            strength = jnp.maximum(strength, jnp.max(reach))
        extent = jnp.float32(0.0)
        for v in range(self.basis_count):
            extent_v = jnp.float32(0.0)
            for frame in range(self.frame_total):
                extent_v = extent_v + jnp.abs(self.basis[v, frame])
            extent = jnp.maximum(extent, extent_v)
        bound = jnp.maximum(sample_bound * extent * strength, 1e-30)
        scale = half_top / jnp.full(shape, bound, jnp.float32)
        self.scale[0] = jnp.max(scale)
        return 1.0 / scale

    def listing(self, slot, local):
        value, inside = self.row_of(local)
        filled = jnp.int32(0)
        doubled = jnp.int32(0)
        again, _ = self.row_of(local)
        for frame in range(self.frame_total):
            taken = (value == self.pattern[frame]) & inside
            self.order[slot * self.frame_total + filled] = frame
            filled = filled + taken.astype(jnp.int32)
            doubled = doubled + (taken & (again != self.pattern[frame])).astype(jnp.int32)
        self.count[2 * slot] = filled
        self.count[2 * slot + 1] = doubled

    def shifted(self, entry):
        narrow = self.source[entry].astype(jnp.bfloat16)
        shifts = [
            lax.rem(self.kx_count - self.offset[tap], self.kx_count)
            for tap in range(self.tap_count)
        ]
        return jnp.concatenate(
            [
                pltpu.roll(narrow[p * self.coil_count : (p + 1) * self.coil_count], shift, axis=1)
                for p in range(2)
                for shift in shifts
            ],
            axis=0,
        )

    def add(self, target, weights, entries):
        for start in range(0, self.parts, sublanes):
            pieces = [
                ref[entry, offset + start : offset + start + sublanes, :]
                for ref, entry, offset in entries
            ]
            for v in range(self.basis_count):
                total = self.totals[target, v, start : start + sublanes, :]
                for weight, piece in zip(weights, pieces):
                    total = total + weight[v] * piece
                self.totals[target, v, start : start + sublanes, :] = total

    def multiply(self, entry, group, tap, offset):
        self.product[entry, offset : offset + self.parts] = jnp.dot(
            self.taps[group, tap * self.parts : (tap + 1) * self.parts],
            self.shifted(entry),
            preferred_element_type=jnp.float32,
        )

    def row(self, slot, local, fetch, targets):
        listed = self.count[2 * slot]
        parts = self.parts
        neighbours = [self.row_of(local + 1 - tap) for tap in range(3)]

        def load(entry, position):
            frame = self.order[slot * self.frame_total + jnp.minimum(position, listed - 1)]
            fetch(entry, frame)
            scale = jnp.where(position < listed, self.scale[0], 0.0)
            direct = [self.basis[v, frame] * scale for v in range(self.basis_count)]
            wanted = self.pattern[frame]
            masked = [
                [jnp.where(inside & (value != wanted), weight, 0.0) for weight in direct]
                for value, inside in neighbours
            ]
            return frame // self.group_frames, direct, masked

        def batch_at(base, size):
            each = range(size)
            loaded = [load(e, base + e) for e in each]
            sides = [tap for tap in (0, 2) if targets[tap] is not None]
            for e in each:
                for tap in sides:
                    self.multiply(e, loaded[e][0], tap, tap // 2 * parts)
            if targets[1] is not None:
                self.add(
                    targets[1], [loaded[e][1] for e in each], [(self.source, e, 0) for e in each]
                )
            for tap in sides:
                self.add(
                    targets[tap],
                    [loaded[e][2][tap] for e in each],
                    [(self.product, e, tap // 2 * parts) for e in each],
                )

        def full(index, carry):
            batch_at(index * batch, batch)
            return carry

        whole = listed // batch
        rest = listed - whole * batch
        large = (rest > batch // 2).astype(jnp.int32)
        lax.fori_loop(0, whole + large, full, 0)

        @pl.when((rest > 0) & (large == 0))
        def _():
            batch_at(whole * batch, batch // 2)

        def centre(index, carry):
            group, _, masked = load(0, index)
            self.multiply(0, group, 1, 0)
            self.add(targets[1], [masked[1]], [(self.product, 0, 0)])
            return carry

        if targets[1] is not None:
            lax.fori_loop(0, jnp.where(self.count[2 * slot + 1] > 0, listed, 0), centre, 0)


def convert_frames(block_ref, samples):
    together, parts, row_count, kx_count = block_ref.shape
    for t in range(together):
        values = block_ref[t].astype(jnp.float32).reshape(parts * row_count, kx_count)
        for half in range(kx_count // lanes):
            samples[pl.program_id(0) * together + t, half] = values[
                :, half * lanes : (half + 1) * lanes
            ]


def list_rows(filler, row_count):
    def listing(row, carry):
        filler.listing(row, row)
        return carry

    lax.fori_loop(0, row_count, listing, 0)


def add_row(filler, samples, row_count, row):
    halves = samples.shape[1]

    def fetch(entry, frame):
        for half in range(halves):
            filler.source[entry, :, half * lanes : (half + 1) * lanes] = samples[
                frame, half, pl.ds(row, filler.parts, stride=row_count), :
            ]

    filler.row(row, row, fetch, (row + 2, row + 1, row))


def pack_rows(filler, own, out_ref, row_at):
    devices, basis_count, stored, _ = out_ref.shape
    held = stored // sublanes

    def pack(index, carry):
        row = row_at(index)
        for v in range(basis_count):
            turned = jnp.concatenate(
                [filler.totals[row + 1, v], filler.totals[row + 2, v]], axis=0
            ).T
            rolled = pltpu.roll(turned, lanes // 2, axis=1)
            turned = turned.reshape(devices, 2, sublanes, lanes)
            rolled = rolled.reshape(devices, 2, sublanes, lanes)
            lower = lax.broadcasted_iota(jnp.int32, (sublanes, lanes), 1) < lanes // 2
            for d in range(devices):
                apart = d ^ own
                slot = (apart & 1) * (devices // 2) + (apart >> 1)
                out_ref[slot, v, pl.ds(2 * index, sublanes, stride=held), :] = jnp.where(
                    lower, turned[d, 0], rolled[d, 1]
                )
                out_ref[slot, v, pl.ds(2 * index + 1, sublanes, stride=held), :] = jnp.where(
                    lower, rolled[d, 0], turned[d, 1]
                )
        return carry

    lax.fori_loop(0, held // 2, pack, 0)


def inner_kernel(
    row_count,
    place_ref,
    pattern_ref,
    segment_ref,
    offset_ref,
    basis_ref,
    block_ref,
    kernel_ref,
    out_ref,
    inverse_ref,
    rest_ref,
    first_ref,
    last_ref,
    samples,
    *scratch,
):
    frame_total, halves, _, _ = samples.shape
    _, parts, _, kx_count = block_ref.shape
    refs = (place_ref, pattern_ref, segment_ref, offset_ref, basis_ref, kernel_ref)
    filler = Filler(refs, scratch, parts, kx_count)
    quarter = row_count // 4
    convert_frames(block_ref, samples)

    @pl.when(pl.program_id(0) == 0)
    def _():
        inverse_ref[...] = filler.prepare(inverse_ref.shape)
        list_rows(filler, row_count)

    @pl.when(pl.program_id(0) == pl.num_programs(0) - 1)
    def _():
        def outer(frame, carry):
            for half in range(halves):
                span = slice(half * lanes, (half + 1) * lanes)
                for ref, row in ((first_ref, 0), (last_ref, row_count - 1)):
                    ref[frame, :, span] = samples[
                        frame, half, pl.ds(row, parts, stride=row_count), :
                    ].astype(jnp.bfloat16)
            return carry

        lax.fori_loop(0, frame_total, outer, 0)

        def rows(index, carry):
            add_row(filler, samples, row_count, index + quarter - 1)
            return carry

        lax.fori_loop(0, 2 * quarter + 2, rows, 0)
        rest_ref[:2] = filler.totals[quarter - 1 : quarter + 1]
        rest_ref[2:] = filler.totals[3 * quarter + 1 : 3 * quarter + 3]
        pack_rows(filler, place_ref[0] // row_count, out_ref, lambda m: 2 * m + quarter)


def outer_kernel(
    row_count,
    place_ref,
    pattern_ref,
    segment_ref,
    offset_ref,
    basis_ref,
    block_ref,
    kernel_ref,
    rest_ref,
    low_ref,
    high_ref,
    out_ref,
    samples,
    *scratch,
):
    _, parts, _, kx_count = block_ref.shape
    refs = (place_ref, pattern_ref, segment_ref, offset_ref, basis_ref, kernel_ref)
    filler = Filler(refs, scratch, parts, kx_count)
    quarter = row_count // 4
    convert_frames(block_ref, samples)

    @pl.when(pl.program_id(0) == 0)
    def _():
        filler.prepare((sublanes, lanes))
        filler.totals[quarter - 1 : quarter + 1] = rest_ref[:2]
        filler.totals[3 * quarter + 1 : 3 * quarter + 3] = rest_ref[2:]
        list_rows(filler, row_count)

    @pl.when(pl.program_id(0) == pl.num_programs(0) - 1)
    def _():
        def rows(index, carry):
            beyond = (index >= quarter - 1).astype(jnp.int32)
            add_row(filler, samples, row_count, index + beyond * (2 * quarter + 2))
            return carry

        lax.fori_loop(0, 2 * quarter - 2, rows, 0)

        sides = (
            (-1, low_ref, (1, None, None)),
            (row_count, high_ref, (None, None, row_count)),
        )
        for local, ref, targets in sides:
            filler.listing(0, local)

            def fetch(entry, frame):
                filler.source[entry] = ref[frame].astype(jnp.float32)

            filler.row(0, local, fetch, targets)

        def row_at(m):
            return 2 * m + (2 * m >= quarter).astype(jnp.int32) * (2 * quarter)

        pack_rows(filler, place_ref[0] // row_count, out_ref, row_at)


def image_kernel(
    row_count, coil_count, place_ref, inverse_ref, inner_ref, outer_ref, table_ref, out_ref, held
):
    devices, _, _, _ = inner_ref.shape
    _, part_count, length, _ = held.shape
    columns = length // coil_count
    parts = part_count * coil_count
    row_total = devices * row_count
    own = place_ref[0] // row_count
    scale = inverse_ref[0:1, 0:1]
    for h, ref in enumerate((inner_ref, outer_ref)):
        for i in range(sublanes):
            turned = jnp.concatenate(
                [ref[d ^ own, 0, i * sublanes : (i + 1) * sublanes, :] for d in range(devices)],
                axis=0,
            ).T
            for j in range(columns // sublanes):
                for p in range(part_count):
                    start = j * parts + p * coil_count
                    held[h, p, pl.ds(j * sublanes + i, coil_count, stride=columns), :] = turned[
                        start : start + coil_count
                    ]
    for start in range(0, length, lanes):
        left = jnp.concatenate(
            [held[h, p, start : start + lanes, :] for p in range(part_count) for h in range(2)],
            axis=1,
        )
        coarse = left.astype(jnp.bfloat16)
        fine = (left - coarse.astype(jnp.float32)).astype(jnp.bfloat16)
        result = jnp.dot(coarse, table_ref[0], preferred_element_type=jnp.float32)
        result = result + jnp.dot(coarse, table_ref[1], preferred_element_type=jnp.float32)
        result = result + jnp.dot(fine, table_ref[0], preferred_element_type=jnp.float32)
        result = result * scale
        for p in range(part_count):
            out_ref[0, p, start : start + lanes, :] = result[:, p * row_total : (p + 1) * row_total]


def inverse_table(row_total, row_count):
    quarter = row_count // 4
    row = np.arange(row_total).reshape(-1, 4, quarter)
    row = np.concatenate([row[:, 1:3].reshape(-1), row[:, 0::3].reshape(-1)])
    index = np.arange(row_total)
    angle = (row[:, None] * index[None, :] % row_total) * (2.0 * np.pi / row_total)
    cosine = np.cos(angle) / np.sqrt(row_total)
    sine = np.sin(angle) / np.sqrt(row_total)
    full = np.block([[cosine, sine], [-sine, cosine]]).astype(np.float32)
    coarse = full.astype(ml_dtypes.bfloat16)
    fine = (full - coarse.astype(np.float32)).astype(ml_dtypes.bfloat16)
    return np.stack([coarse, fine])


def on_device(kspace, kernel, pattern, offsets, segment, temporal_basis):
    frame_total, part_count, coil_count, row_count, kx_count = kspace.shape
    devices = lax.axis_size("ky")
    columns = kx_count // devices
    parts = part_count * coil_count
    row_total = row_count * devices
    tap_count = offsets.shape[0]
    fits = (
        2 * parts == lanes
        and row_count == 2 * sublanes
        and columns == 2 * sublanes
        and row_total == 2 * lanes
        and kx_count % lanes == 0
        and tap_count * coil_count == lanes
        and frame_total % together == 0
        and devices & (devices - 1) == 0
    )
    if not fits:
        return plain_device(kspace, kernel, pattern, offsets, segment, temporal_basis)

    basis_count = temporal_basis.shape[0]
    group_count = kernel.shape[0]
    stored = sublanes * row_count // 2
    halves = kx_count // lanes
    edge_shape = (frame_total, parts, kx_count)
    payload_shape = (devices, basis_count, stored, lanes)

    place = (lax.axis_index("ky") * row_count).astype(jnp.int32).reshape(1)
    kernel_rows = kernel.transpose(0, 2, 1)
    fill_work = 2 * frame_total * row_count * kx_count * kernel.shape[1] * parts
    estimate = pl.CostEstimate(flops=fill_work, bytes_accessed=0, transcendentals=0)
    scalars = (place, pattern, segment, offsets, temporal_basis)
    samples = kspace.reshape(frame_total, parts, row_count, kx_count)
    scalar = pl.BlockSpec(memory_space=pltpu.SMEM)

    def whole(shape):
        return pl.BlockSpec(shape, lambda t: (0,) * len(shape))

    in_specs = [scalar] * len(scalars) + [
        pl.BlockSpec((together, parts, row_count, kx_count), lambda t: (t, 0, 0, 0)),
        whole(kernel_rows.shape),
    ]
    scratch_shapes = [
        pltpu.VMEM((frame_total, halves, parts * row_count, lanes), jnp.float32),
        pltpu.VMEM((batch, parts, kx_count), jnp.float32),
        pltpu.VMEM((batch, 2 * parts, kx_count), jnp.float32),
        pltpu.VMEM((row_count + 2, basis_count, parts, kx_count), jnp.float32),
        pltpu.VMEM((group_count, 3 * parts, tap_count * parts), jnp.bfloat16),
        pltpu.SMEM((row_count * frame_total + 1,), jnp.int32),
        pltpu.SMEM((2 * row_count,), jnp.int32),
        pltpu.SMEM((1,), jnp.float32),
    ]
    inner_shapes = [
        jax.ShapeDtypeStruct(payload_shape, jnp.float32),
        jax.ShapeDtypeStruct((sublanes, lanes), jnp.float32),
        jax.ShapeDtypeStruct((4, basis_count, parts, kx_count), jnp.float32),
        jax.ShapeDtypeStruct(edge_shape, jnp.bfloat16),
        jax.ShapeDtypeStruct(edge_shape, jnp.bfloat16),
    ]
    inner, inverse, rest, first, last = pl.pallas_call(
        functools.partial(inner_kernel, row_count),
        grid=(frame_total // together,),
        in_specs=in_specs,
        out_specs=[whole(shape.shape) for shape in inner_shapes],
        out_shape=inner_shapes,
        scratch_shapes=scratch_shapes,
        cost_estimate=estimate,
        name="inner",
    )(*scalars, samples, kernel_rows)
    low = lax.ppermute(last, "ky", [(i, i + 1) for i in range(devices - 1)])
    high = lax.ppermute(first, "ky", [(i + 1, i) for i in range(devices - 1)])

    def swap(block, distance):
        return lax.ppermute(block, "ky", [(i, i ^ distance) for i in range(devices)])

    chips = devices // 2

    def paired(payload):
        payload = payload.astype(jnp.float16)
        partner = swap(payload[chips:], 1)
        return [jnp.stack([payload[m], partner[m]]) for m in range(chips)]

    def gathered(pairs, received):
        return jnp.concatenate([pairs[0]] + received).astype(jnp.float32)

    inner_pairs = paired(inner)
    inner_pairs, held_place = lax.optimization_barrier((inner_pairs, place))
    inner_received = []
    for m in range(1, chips):
        inner_received.append(swap(inner_pairs[m], 2 * m))
    outer = pl.pallas_call(
        functools.partial(outer_kernel, row_count),
        grid=(frame_total // together,),
        in_specs=in_specs + [whole(rest.shape), whole(edge_shape), whole(edge_shape)],
        out_specs=whole(payload_shape),
        out_shape=jax.ShapeDtypeStruct(payload_shape, jnp.float32),
        scratch_shapes=scratch_shapes,
        cost_estimate=estimate,
        name="outer",
    )(held_place, *scalars[1:], samples, kernel_rows, rest, low, high)
    outer_pairs = paired(outer)
    outer_received = [swap(outer_pairs[m], 2 * m) for m in range(1, chips)]
    inner = gathered(inner_pairs, inner_received)
    outer = gathered(outer_pairs, outer_received)

    table = jnp.asarray(inverse_table(row_total, row_count))
    length = coil_count * columns
    images = pl.pallas_call(
        functools.partial(image_kernel, row_count, coil_count),
        grid=(basis_count,),
        in_specs=[
            scalar,
            pl.BlockSpec((sublanes, lanes), lambda v: (0, 0)),
            pl.BlockSpec((devices, 1, stored, lanes), lambda v: (0, v, 0, 0)),
            pl.BlockSpec((devices, 1, stored, lanes), lambda v: (0, v, 0, 0)),
            pl.BlockSpec(table.shape, lambda v: (0, 0, 0)),
        ],
        out_specs=pl.BlockSpec((1, part_count, length, row_total), lambda v: (v, 0, 0, 0)),
        out_shape=jax.ShapeDtypeStruct(
            (basis_count, part_count, length, row_total), jnp.float32
        ),
        scratch_shapes=[
            pltpu.VMEM((2, part_count, length, row_total // 2), jnp.float32)
        ],
        name="image",
    )(place, inverse, inner, outer, table)
    return images.reshape(basis_count, part_count, coil_count, columns, row_total)


def solution(mesh):
    return jax.shard_map(
        on_device,
        mesh=mesh,
        in_specs=(P("study", None, None, "ky", None), P(), P("study"), P(), P(), P()),
        out_specs=P("study", None, None, "ky", None),
        check_vma=False,
    )
```

```python
import functools

import jax
import jax.numpy as jnp
import ml_dtypes
import numpy as np
from jax import lax
from jax.experimental import pallas as pl
from jax.experimental.pallas import tpu as pltpu
from jax.sharding import PartitionSpec as P


frame_block = 4
batch = 4
together = 8
tall = 4
sample_bound = 6.0
half_top = 60000.0
lanes = 128
sublanes = 8


def padded_2(block, sides, width):
    for axis, dim in sides:
        count = lax.axis_size(axis)
        forward = [(i, i + 1) for i in range(count - 1)]
        backward = [(target, source) for source, target in forward]
        low = lax.ppermute(
            lax.slice_in_dim(block, block.shape[dim] - width, None, axis=dim), axis, forward
        )
        high = lax.ppermute(lax.slice_in_dim(block, 0, width, axis=dim), axis, backward)
        block = jnp.concatenate([low, block, high], axis=dim)
    return block


def inverse_rows(spectra):
    row_total = spectra.shape[3]
    row_index = jnp.arange(row_total, dtype=jnp.int32)
    phase_index = row_index[:, None] * row_index[None, :] % row_total
    phase_angle = phase_index.astype(jnp.float32) * (2.0 * jnp.pi / row_total)
    cosine_table = jnp.cos(phase_angle)
    sine_table = jnp.sin(phase_angle)
    real_part = spectra[:, 0]
    imag_part = spectra[:, 1]
    high = lax.Precision.HIGHEST
    out_real = jnp.einsum("yk,mckx->mcxy", cosine_table, real_part, precision=high) - jnp.einsum(
        "yk,mckx->mcxy", sine_table, imag_part, precision=high
    )
    out_imag = jnp.einsum("yk,mckx->mcxy", sine_table, real_part, precision=high) + jnp.einsum(
        "yk,mckx->mcxy", cosine_table, imag_part, precision=high
    )
    scale = 1.0 / jnp.sqrt(jnp.float32(row_total))
    return jnp.stack([out_real, out_imag], axis=1) * scale


def plain_device(kspace, kernel, pattern, offsets, segment, temporal_basis):
    frame_total, _, coil_count, row_count, kx_count = kspace.shape
    group_count = kernel.shape[0]
    group_frames = frame_total // group_count
    row_start = lax.axis_index("ky") * row_count
    local_segment = lax.dynamic_slice_in_dim(segment, row_start, row_count)
    acquired = (local_segment[None, :] == pattern[:, None])[:, None, None, :, None]
    zero_fill = jnp.where(acquired, kspace, jnp.zeros_like(kspace))
    padded = padded_2(zero_fill, (("ky", 3),), 1)
    blocks = frame_total // frame_block
    padded_blocks = padded.reshape(blocks, frame_block, 2, coil_count, row_count + 2, kx_count)
    block_group = jnp.arange(blocks, dtype=jnp.int32) * frame_block // group_frames

    def estimate_block(block_item):
        block_data, group_index = block_item
        ky_layers = []
        for ky_tap in range(3):
            ky_slice = block_data[:, :, :, ky_tap : ky_tap + row_count, :]
            ky_layers.append(
                jnp.stack(
                    [
                        jnp.roll(ky_slice, -offsets[kx_tap], axis=4)
                        for kx_tap in range(offsets.shape[0])
                    ],
                    axis=2,
                )
            )
        sources = jnp.stack(ky_layers, axis=2).reshape(frame_block, -1, row_count * kx_count)
        weights = lax.dynamic_index_in_dim(kernel, group_index, 0, keepdims=False)
        return jnp.einsum("io,fir->for", weights, sources, preferred_element_type=jnp.float32)

    estimate = lax.map(estimate_block, (padded_blocks, block_group))
    estimate = estimate.reshape(frame_total, 2, coil_count, row_count, kx_count)
    filled = jnp.where(acquired, kspace.astype(jnp.float32), estimate)
    high = lax.Precision.HIGHEST
    coefficients = jnp.einsum("bf,fpcrx->bpcrx", temporal_basis, filled, precision=high)
    swapped = lax.all_to_all(coefficients, "ky", split_axis=4, concat_axis=3, tiled=True)
    return inverse_rows(swapped)


class Filler:

    def __init__(self, refs, scratch, taps, parts, kx_count):
        self.place, self.pattern, self.segment, self.offset, self.basis, self.kernel = refs
        self.source, self.product, self.totals, self.order, self.count, self.scale = scratch
        self.taps = taps
        self.parts = parts
        self.kx_count = kx_count
        self.frame_total = self.pattern.shape[0]
        self.row_total = self.segment.shape[0]
        self.basis_count = self.basis.shape[0]
        self.group_count = self.kernel.shape[0]
        self.group_frames = self.frame_total // self.group_count
        self.tap_count = self.offset.shape[0]
        self.coil_count = parts // 2

    def row_of(self, local):
        row = self.place[0] + local
        inside = (row >= 0) & (row < self.row_total)
        return self.segment[jnp.clip(row, 0, self.row_total - 1)], inside

    def prepare(self, shape):
        width = self.tap_count * self.coil_count
        strength = jnp.float32(1.0)
        for group in range(self.group_count):
            for tap in range(3):
                joined = jnp.concatenate(
                    [
                        self.kernel[group, :, (p * 3 + tap) * width : (p * 3 + tap + 1) * width]
                        for p in range(2)
                    ],
                    axis=1,
                )
                self.taps[group, tap * self.parts : (tap + 1) * self.parts, :] = joined
            reach = jnp.sum(jnp.abs(self.kernel[group].astype(jnp.float32)), axis=1, keepdims=True)
            strength = jnp.maximum(strength, jnp.max(reach))
        extent = jnp.float32(0.0)
        for v in range(self.basis_count):
            extent_v = jnp.float32(0.0)
            for frame in range(self.frame_total):
                extent_v = extent_v + jnp.abs(self.basis[v, frame])
            extent = jnp.maximum(extent, extent_v)
        bound = jnp.maximum(sample_bound * extent * strength, 1e-30)
        scale = half_top / jnp.full(shape, bound, jnp.float32)
        self.scale[0] = jnp.max(scale)
        return scale

    def listing(self, slot, local):
        value, inside = self.row_of(local)
        filled = jnp.int32(0)
        doubled = jnp.int32(0)
        again, _ = self.row_of(local)
        for frame in range(self.frame_total):
            taken = (value == self.pattern[frame]) & inside
            self.order[slot * self.frame_total + filled] = frame
            filled = filled + taken.astype(jnp.int32)
            doubled = doubled + (taken & (again != self.pattern[frame])).astype(jnp.int32)
        self.count[2 * slot] = filled
        self.count[2 * slot + 1] = doubled

    def shifted(self, entry):
        narrow = self.source[entry].astype(jnp.bfloat16)
        shifts = [
            lax.rem(self.kx_count - self.offset[tap], self.kx_count)
            for tap in range(self.tap_count)
        ]
        return jnp.concatenate(
            [
                pltpu.roll(narrow[p * self.coil_count : (p + 1) * self.coil_count], shift, axis=1)
                for p in range(2)
                for shift in shifts
            ],
            axis=0,
        )

    def add(self, target, weights, entries):
        for start in range(0, self.parts, sublanes):
            pieces = [
                ref[entry, offset + start : offset + start + sublanes, :]
                for ref, entry, offset in entries
            ]
            for v in range(self.basis_count):
                total = self.totals[target, v, start : start + sublanes, :]
                for weight, piece in zip(weights, pieces):
                    total = total + weight[v] * piece
                self.totals[target, v, start : start + sublanes, :] = total

    def multiply(self, entry, group, tap, offset):
        self.product[entry, offset : offset + self.parts] = jnp.dot(
            self.taps[group, tap * self.parts : (tap + 1) * self.parts],
            self.shifted(entry),
            preferred_element_type=jnp.float32,
        )

    def row(self, slot, local, fetch, targets):
        listed = self.count[2 * slot]
        parts = self.parts
        neighbours = [self.row_of(local + 1 - tap) for tap in range(3)]

        def load(entry, position):
            frame = self.order[slot * self.frame_total + jnp.minimum(position, listed - 1)]
            fetch(entry, frame)
            scale = jnp.where(position < listed, self.scale[0], 0.0)
            direct = [self.basis[v, frame] * scale for v in range(self.basis_count)]
            wanted = self.pattern[frame]
            masked = [
                [jnp.where(inside & (value != wanted), weight, 0.0) for weight in direct]
                for value, inside in neighbours
            ]
            return frame // self.group_frames, direct, masked

        def batch_at(base, size):
            each = range(size)
            loaded = [load(e, base + e) for e in each]
            sides = [tap for tap in (0, 2) if targets[tap] is not None]
            for e in each:
                for tap in sides:
                    self.multiply(e, loaded[e][0], tap, tap // 2 * parts)
            if targets[1] is not None:
                self.add(
                    targets[1], [loaded[e][1] for e in each], [(self.source, e, 0) for e in each]
                )
            for tap in sides:
                self.add(
                    targets[tap],
                    [loaded[e][2][tap] for e in each],
                    [(self.product, e, tap // 2 * parts) for e in each],
                )

        def full(index, carry):
            batch_at(index * batch, batch)
            return carry

        whole = listed // batch
        rest = listed - whole * batch
        large = (rest > batch // 2).astype(jnp.int32)
        lax.fori_loop(0, whole + large, full, 0)

        @pl.when((rest > 0) & (large == 0))
        def _():
            batch_at(whole * batch, batch // 2)

        def centre(index, carry):
            group, _, masked = load(0, index)
            self.multiply(0, group, 1, 0)
            self.add(targets[1], [masked[1]], [(self.product, 0, 0)])
            return carry

        if targets[1] is not None:
            lax.fori_loop(0, jnp.where(self.count[2 * slot + 1] > 0, listed, 0), centre, 0)


def convert_frames(block_ref, samples):
    together, parts, row_count, kx_count = block_ref.shape
    for t in range(together):
        values = block_ref[t].astype(jnp.float32).reshape(parts * row_count, kx_count)
        for half in range(kx_count // lanes):
            samples[pl.program_id(0) * together + t, half] = values[
                :, half * lanes : (half + 1) * lanes
            ]


def list_rows(filler, start, stop):
    def listing(row, carry):
        filler.listing(row, row)
        return carry

    lax.fori_loop(start, stop, listing, 0)


def clear_rows(filler, start, stop):
    shape = (stop - start,) + filler.totals.shape[1:]
    filler.totals[start + 1 : stop + 1] = jnp.zeros(shape, jnp.float32)


def add_row(filler, samples, row_count, row):
    halves = samples.shape[1]

    def fetch(entry, frame):
        for half in range(halves):
            filler.source[entry, :, half * lanes : (half + 1) * lanes] = samples[
                frame, half, pl.ds(row, filler.parts, stride=row_count), :
            ]

    filler.row(row, row, fetch, (row + 2, row + 1, row))


def pack_rows(filler, own, out_ref, row_at):
    devices, basis_count, stored, _ = out_ref.shape
    held = stored // sublanes

    def pack(index, carry):
        row = row_at(index)
        for v in range(basis_count):
            turned = jnp.concatenate(
                [filler.totals[row + 1, v], filler.totals[row + 2, v]], axis=0
            ).T
            rolled = pltpu.roll(turned, lanes // 2, axis=1)
            turned = turned.reshape(devices, 2, sublanes, lanes)
            rolled = rolled.reshape(devices, 2, sublanes, lanes)
            lower = lax.broadcasted_iota(jnp.int32, (sublanes, lanes), 1) < lanes // 2
            for d in range(devices):
                apart = d ^ own
                slot = (apart & 1) * (devices // 2) + (apart >> 1)
                out_ref[slot, v, pl.ds(2 * index, sublanes, stride=held), :] = jnp.where(
                    lower, turned[d, 0], rolled[d, 1]
                )
                out_ref[slot, v, pl.ds(2 * index + 1, sublanes, stride=held), :] = jnp.where(
                    lower, rolled[d, 0], turned[d, 1]
                )
        return carry

    lax.fori_loop(0, held // 2, pack, 0)


def inner_kernel(
    row_count,
    place_ref,
    pattern_ref,
    segment_ref,
    offset_ref,
    basis_ref,
    block_ref,
    kernel_ref,
    out_ref,
    scale_ref,
    rest_ref,
    first_ref,
    last_ref,
    taps_ref,
    samples,
    *scratch,
):
    frame_total, halves, _, _ = samples.shape
    _, parts, _, kx_count = block_ref.shape
    refs = (place_ref, pattern_ref, segment_ref, offset_ref, basis_ref, kernel_ref)
    filler = Filler(refs, scratch, taps_ref, parts, kx_count)
    quarter = row_count // 4
    convert_frames(block_ref, samples)

    @pl.when(pl.program_id(0) == 0)
    def _():
        scale_ref[...] = filler.prepare(scale_ref.shape)
        clear_rows(filler, quarter - 2, 3 * quarter + 2)
        list_rows(filler, quarter - 1, 3 * quarter + 1)

    @pl.when(pl.program_id(0) == pl.num_programs(0) - 1)
    def _():
        def outer(frame, carry):
            for half in range(halves):
                span = slice(half * lanes, (half + 1) * lanes)
                for ref, row in ((first_ref, 0), (last_ref, row_count - 1)):
                    ref[frame, :, span] = samples[
                        frame, half, pl.ds(row, parts, stride=row_count), :
                    ].astype(jnp.bfloat16)
            return carry

        lax.fori_loop(0, frame_total, outer, 0)

        def rows(index, carry):
            add_row(filler, samples, row_count, index + quarter - 1)
            return carry

        lax.fori_loop(0, 2 * quarter + 2, rows, 0)
        rest_ref[:2] = filler.totals[quarter - 1 : quarter + 1]
        rest_ref[2:] = filler.totals[3 * quarter + 1 : 3 * quarter + 3]
        pack_rows(filler, place_ref[0] // row_count, out_ref, lambda m: 2 * m + quarter)


def outer_kernel(
    row_count,
    place_ref,
    pattern_ref,
    segment_ref,
    offset_ref,
    basis_ref,
    block_ref,
    kernel_ref,
    scale_ref,
    taps_ref,
    rest_ref,
    low_ref,
    high_ref,
    out_ref,
    samples,
    *scratch,
):
    _, parts, _, kx_count = block_ref.shape
    refs = (place_ref, pattern_ref, segment_ref, offset_ref, basis_ref, kernel_ref)
    filler = Filler(refs, scratch, taps_ref, parts, kx_count)
    quarter = row_count // 4
    convert_frames(block_ref, samples)

    @pl.when(pl.program_id(0) == 0)
    def _():
        filler.scale[0] = jnp.max(scale_ref[...])
        clear_rows(filler, 0, quarter - 2)
        clear_rows(filler, 3 * quarter + 2, row_count)
        filler.totals[quarter - 1 : quarter + 1] = rest_ref[:2]
        filler.totals[3 * quarter + 1 : 3 * quarter + 3] = rest_ref[2:]
        list_rows(filler, 0, quarter - 1)
        list_rows(filler, 3 * quarter + 1, row_count)

    @pl.when(pl.program_id(0) == pl.num_programs(0) - 1)
    def _():
        def rows(index, carry):
            beyond = (index >= quarter - 1).astype(jnp.int32)
            add_row(filler, samples, row_count, index + beyond * (2 * quarter + 2))
            return carry

        lax.fori_loop(0, 2 * quarter - 2, rows, 0)

        sides = (
            (-1, low_ref, (1, None, None)),
            (row_count, high_ref, (None, None, row_count)),
        )
        for local, ref, targets in sides:
            filler.listing(0, local)

            def fetch(entry, frame):
                filler.source[entry] = ref[frame].astype(jnp.float32)

            filler.row(0, local, fetch, targets)

        def row_at(m):
            return 2 * m + (2 * m >= quarter).astype(jnp.int32) * (2 * quarter)

        pack_rows(filler, place_ref[0] // row_count, out_ref, row_at)


def image_kernel(
    row_count, coil_count, place_ref, scale_ref, inner_ref, outer_ref, table_ref, out_ref, held
):
    devices, _, _, _ = inner_ref.shape
    _, part_count, length, _ = held.shape
    columns = length // coil_count
    parts = part_count * coil_count
    row_total = devices * row_count
    own = place_ref[0] // row_count
    scale = 1.0 / scale_ref[0:1, 0:1]
    for h, ref in enumerate((inner_ref, outer_ref)):
        for i in range(sublanes):
            turned = jnp.concatenate(
                [ref[d ^ own, 0, i * sublanes : (i + 1) * sublanes, :] for d in range(devices)],
                axis=0,
            ).T
            for j in range(columns // sublanes):
                for p in range(part_count):
                    start = j * parts + p * coil_count
                    held[h, p, pl.ds(j * sublanes + i, coil_count, stride=columns), :] = turned[
                        start : start + coil_count
                    ]
    span = tall * lanes
    for start in range(0, length, span):
        left = jnp.concatenate(
            [held[h, p, start : start + span, :] for p in range(part_count) for h in range(2)],
            axis=1,
        )
        coarse = left.astype(jnp.bfloat16)
        fine = (left - coarse.astype(jnp.float32)).astype(jnp.bfloat16)
        result = jnp.dot(coarse, table_ref[0], preferred_element_type=jnp.float32)
        result = result + jnp.dot(coarse, table_ref[1], preferred_element_type=jnp.float32)
        result = result + jnp.dot(fine, table_ref[0], preferred_element_type=jnp.float32)
        result = result * scale
        for p in range(part_count):
            out_ref[0, p, start : start + span, :] = result[:, p * row_total : (p + 1) * row_total]


def inverse_table(row_total, row_count):
    quarter = row_count // 4
    row = np.arange(row_total).reshape(-1, 4, quarter)
    row = np.concatenate([row[:, 1:3].reshape(-1), row[:, 0::3].reshape(-1)])
    index = np.arange(row_total)
    angle = (row[:, None] * index[None, :] % row_total) * (2.0 * np.pi / row_total)
    cosine = np.cos(angle) / np.sqrt(row_total)
    sine = np.sin(angle) / np.sqrt(row_total)
    full = np.block([[cosine, sine], [-sine, cosine]]).astype(np.float32)
    coarse = full.astype(ml_dtypes.bfloat16)
    fine = (full - coarse.astype(np.float32)).astype(ml_dtypes.bfloat16)
    return np.stack([coarse, fine])


def on_device(kspace, kernel, pattern, offsets, segment, temporal_basis):
    frame_total, part_count, coil_count, row_count, kx_count = kspace.shape
    devices = lax.axis_size("ky")
    columns = kx_count // devices
    parts = part_count * coil_count
    row_total = row_count * devices
    tap_count = offsets.shape[0]
    fits = (
        2 * parts == lanes
        and row_count == 2 * sublanes
        and columns == 2 * sublanes
        and row_total == 2 * lanes
        and kx_count % lanes == 0
        and tap_count * coil_count == lanes
        and frame_total % together == 0
        and devices & (devices - 1) == 0
    )
    if not fits:
        return plain_device(kspace, kernel, pattern, offsets, segment, temporal_basis)

    basis_count = temporal_basis.shape[0]
    group_count = kernel.shape[0]
    stored = sublanes * row_count // 2
    halves = kx_count // lanes
    edge_shape = (frame_total, parts, kx_count)
    payload_shape = (devices, basis_count, stored, lanes)

    place = (lax.axis_index("ky") * row_count).astype(jnp.int32).reshape(1)
    kernel_rows = kernel.transpose(0, 2, 1)
    fill_work = 2 * frame_total * row_count * kx_count * kernel.shape[1] * parts
    estimate = pl.CostEstimate(flops=fill_work, bytes_accessed=0, transcendentals=0)
    scalars = (place, pattern, segment, offsets, temporal_basis)
    samples = kspace.reshape(frame_total, parts, row_count, kx_count)
    scalar = pl.BlockSpec(memory_space=pltpu.SMEM)

    def whole(shape):
        return pl.BlockSpec(shape, lambda t: (0,) * len(shape))

    in_specs = [scalar] * len(scalars) + [
        pl.BlockSpec((together, parts, row_count, kx_count), lambda t: (t, 0, 0, 0)),
        whole(kernel_rows.shape),
    ]
    scratch_shapes = [
        pltpu.VMEM((frame_total, halves, parts * row_count, lanes), jnp.float32),
        pltpu.VMEM((batch, parts, kx_count), jnp.float32),
        pltpu.VMEM((batch, 2 * parts, kx_count), jnp.float32),
        pltpu.VMEM((row_count + 2, basis_count, parts, kx_count), jnp.float32),
        pltpu.SMEM((row_count * frame_total + 1,), jnp.int32),
        pltpu.SMEM((2 * row_count,), jnp.int32),
        pltpu.SMEM((1,), jnp.float32),
    ]
    inner_shapes = [
        jax.ShapeDtypeStruct(payload_shape, jnp.float32),
        jax.ShapeDtypeStruct((sublanes, lanes), jnp.float32),
        jax.ShapeDtypeStruct((4, basis_count, parts, kx_count), jnp.float32),
        jax.ShapeDtypeStruct(edge_shape, jnp.bfloat16),
        jax.ShapeDtypeStruct(edge_shape, jnp.bfloat16),
        jax.ShapeDtypeStruct((group_count, 3 * parts, tap_count * parts), jnp.bfloat16),
    ]
    inner, scale, rest, first, last, taps = pl.pallas_call(
        functools.partial(inner_kernel, row_count),
        grid=(frame_total // together,),
        in_specs=in_specs,
        out_specs=[whole(shape.shape) for shape in inner_shapes],
        out_shape=inner_shapes,
        scratch_shapes=scratch_shapes,
        cost_estimate=estimate,
        name="inner",
    )(*scalars, samples, kernel_rows)
    low = lax.ppermute(last, "ky", [(i, i + 1) for i in range(devices - 1)])
    high = lax.ppermute(first, "ky", [(i + 1, i) for i in range(devices - 1)])

    def swap(block, distance):
        return lax.ppermute(block, "ky", [(i, i ^ distance) for i in range(devices)])

    chips = devices // 2

    def paired(payload):
        payload = payload.astype(jnp.float16)
        partner = swap(payload[chips:], 1)
        return [jnp.stack([payload[m], partner[m]]) for m in range(chips)]

    def gathered(pairs, received):
        return jnp.concatenate([pairs[0]] + received).astype(jnp.float32)

    inner_pairs = paired(inner)
    inner_pairs, held_place = lax.optimization_barrier((inner_pairs, place))
    inner_received = []
    for m in range(1, chips):
        inner_received.append(swap(inner_pairs[m], 2 * m))
    outer = pl.pallas_call(
        functools.partial(outer_kernel, row_count),
        grid=(frame_total // together,),
        in_specs=in_specs
        + [whole(array.shape) for array in (scale, taps, rest, low, high)],
        out_specs=whole(payload_shape),
        out_shape=jax.ShapeDtypeStruct(payload_shape, jnp.float32),
        scratch_shapes=scratch_shapes,
        cost_estimate=estimate,
        name="outer",
    )(held_place, *scalars[1:], samples, kernel_rows, scale, taps, rest, low, high)
    outer_pairs = paired(outer)
    outer_received = []
    for m in range(1, chips):
        outer_received.append(swap(outer_pairs[m], 2 * m))
    inner = gathered(inner_pairs, inner_received)
    outer = gathered(outer_pairs, outer_received)

    table = jnp.asarray(inverse_table(row_total, row_count))
    length = coil_count * columns
    images = pl.pallas_call(
        functools.partial(image_kernel, row_count, coil_count),
        grid=(basis_count,),
        in_specs=[
            scalar,
            pl.BlockSpec((sublanes, lanes), lambda v: (0, 0)),
            pl.BlockSpec((devices, 1, stored, lanes), lambda v: (0, v, 0, 0)),
            pl.BlockSpec((devices, 1, stored, lanes), lambda v: (0, v, 0, 0)),
            pl.BlockSpec(table.shape, lambda v: (0, 0, 0)),
        ],
        out_specs=pl.BlockSpec((1, part_count, length, row_total), lambda v: (v, 0, 0, 0)),
        out_shape=jax.ShapeDtypeStruct(
            (basis_count, part_count, length, row_total), jnp.float32
        ),
        scratch_shapes=[
            pltpu.VMEM((2, part_count, length, row_total // 2), jnp.float32)
        ],
        name="image",
    )(place, scale, inner, outer, table)
    return images.reshape(basis_count, part_count, coil_count, columns, row_total)


def solution(mesh):
    return jax.shard_map(
        on_device,
        mesh=mesh,
        in_specs=(P("study", None, None, "ky", None), P(), P("study"), P(), P(), P()),
        out_specs=P("study", None, None, "ky", None),
        check_vma=False,
    )
```
